32 devices in a mesh: gx: 4 (over y, x), gy: 2 (over core), gz: 4 (over z).
Axes of the slice: x: 2, y: 2, z: 4, core: 2. Of those that a mesh axis runs over, the one named last changes fastest.
Arguments:
- gradient: bfloat16 [32, 32, 16, 512], P(None, 'gx', 'gy', 'gz'), may hold values from -6 to 6
- noise_draw: bfloat16 [32, 32, 16, 512], P(None, 'gx', 'gy', 'gz'), may hold values from -6 to 6
- current: float32 [32, 32, 16, 512], P(None, 'gx', 'gy', 'gz'), may hold values from -6 to 6
- eigvectors: bfloat16 [32, 16, 512, 512], P('gx', 'gy', 'gz'), may hold values from -0.125 to 0.125
- eigvalues: float32 [512], replicated, may hold values from 0.05 to 50
- reaction: float32 [32, 16, 512], P('gx', 'gy', 'gz'), may hold values from 0.25 to 4
Outputs:
- proposal: float32 [32, 32, 16, 512], P(None, 'gx', 'gy', 'gz')
The draws below stay inside these ranges and needn't reach their ends.
All inputs are finite; a program needn't handle non-finite values.
Results may differ from the reference program's by a relative error of at most 0.00031.
Values sent between devices are 32-bit elements; how exact they have to be, the bound alone decides.
No kernel may reach another device: no remote copies, remote signals or barrier semaphores. Data moves between devices by JAX's collectives and lax.ppermute only.
A program may use at most 64 MiB of HBM per device.

```python
import math
import jax
import jax.numpy as jnp
from jax import lax

R = 512
CHAINS = 32
SWEEPS = 4
NX = 32
NY = 16
NZ = 512


def block_scale(stream_key, dims, cuts, least, largest):
    loudness, own = 1.0, jax.random.fold_in(stream_key, 6)
    for dim, parts in cuts:
        heights = jnp.exp(jax.random.uniform(jax.random.fold_in(own, dim), (parts,), jnp.float32, least / len(cuts), largest / len(cuts)))
        loudness = loudness * jnp.repeat(heights, dims[dim] // parts).reshape([-1 if axis == dim else 1 for axis in range(len(dims))])
    return loudness


def normal_values(rng, shape, spread, reach, cuts=(), kind=jnp.bfloat16):
    entries = jax.random.normal(rng, shape, jnp.float32) * spread
    if len(cuts) > 0:
        entries = block_scale(rng, shape, cuts, -0.22, 0.18) * entries
    return jnp.clip(entries, min=-reach, max=reach).astype(kind)


def setup_inputs(seed: int = 0) -> dict:
    streams_of = jax.random.split(jax.random.key(seed), 7)
    gradient = normal_values(streams_of[0], (CHAINS, NX, NY, NZ), 1.0, 6.0, ((1, 4), (2, 2), (3, 4)))
    noise_draw = normal_values(streams_of[1], (CHAINS, NX, NY, NZ), 1.0, 6.0, ((1, 4), (2, 2), (3, 4)))
    current = normal_values(streams_of[2], (CHAINS, NX, NY, NZ), 1.0, 6.0, ((1, 4), (2, 2), (3, 4)), jnp.float32)
    eigvectors = normal_values(streams_of[3], (NX, NY, NZ, R), ((R * NX * NY * NZ) ** -0.25), 0.125, ((0, 4), (1, 2), (2, 4)))
    eigvalues = jnp.clip(jnp.exp(jax.random.uniform(streams_of[4], (R,), jnp.float32, math.log(0.05), math.log(50.0))), 0.05, 50.0)
    reaction = jnp.clip(jnp.exp(math.log(4.0) - 2.7725887 * jax.random.uniform(streams_of[5], (NX, NY, NZ), jnp.float32) ** block_scale(streams_of[5], (NX, NY, NZ), ((0, 4), (1, 2), (2, 4)), -0.2, 0.2)), 0.25, 4.0)
    return dict(gradient=gradient, noise_draw=noise_draw, current=current, eigvectors=eigvectors, eigvalues=eigvalues, reaction=reaction)


def neighbours(field):
    padded = jnp.pad(field, ((0, 0), (1, 1), (1, 1), (1, 1)))
    total = padded[:, 2:, 1:-1, 1:-1] + padded[:, :-2, 1:-1, 1:-1]
    total = total + padded[:, 1:-1, 2:, 1:-1] + padded[:, 1:-1, :-2, 1:-1]
    total = total + padded[:, 1:-1, 1:-1, 2:] + padded[:, 1:-1, 1:-1, :-2]
    return total

def reference(gradient, noise_draw, current, eigvectors, eigvalues, reaction):
    stacked = jnp.concatenate([gradient, noise_draw], 0)
    slabs = jnp.moveaxis(stacked, 1, 0)

    def accumulate(total, pair):
        basis_slab, data_slab = pair
        rows = basis_slab.reshape(-1, R)
        vectors = data_slab.reshape(data_slab.shape[0], -1)
        return (total + jnp.dot(vectors, rows, preferred_element_type=jnp.float32), None)
    start = jnp.zeros((2 * CHAINS, R), jnp.float32)
    sums, _ = lax.scan(accumulate, start, (eigvectors, slabs))
    proj_grad = sums[:CHAINS]
    proj_noise = sums[CHAINS:]
    damp = eigvalues / (eigvalues + 1.0)
    root_damp = 1.0 - 1.0 / jnp.sqrt(1.0 + eigvalues)
    coef = (0.5 * damp * proj_grad - 1.0 * root_damp * proj_noise).astype(jnp.bfloat16)

    def expand(basis_slab):
        rows = basis_slab.reshape(-1, R)
        return lax.dot_general(coef, rows, (((1,), (1,)), ((), ())), preferred_element_type=jnp.float32)
    corr_slabs = lax.map(expand, eigvectors)
    corr = jnp.moveaxis(corr_slabs, 0, 1).reshape(current.shape)
    source = -0.5 * gradient.astype(jnp.float32) + 1.0 * noise_draw.astype(jnp.float32) + corr
    diagonal = reaction + 6.0
    field = source / diagonal
    for sweep_index in range(SWEEPS - 1):
        field = (source + neighbours(field)) / diagonal
    return current + field
```

```python
import jax
import jax.numpy as jnp
from jax import lax
from jax.experimental import pallas as pl
from jax.experimental.pallas import tpu as pltpu
from jax.sharding import PartitionSpec as P

SWEEPS = 4


def reduce_over(value, axis):
    count = lax.axis_size(axis)
    if count & (count - 1):
        return lax.psum(value, axis)
    step = 1
    while step < count:
        value = value + lax.ppermute(value, axis, [(i, i ^ step) for i in range(count)])
        step *= 2
    return value


def lines(axis):
    count = lax.axis_size(axis)
    forward = [(i, i + 1) for i in range(count - 1)]
    return forward, [(target, source) for source, target in forward]


def put_column(packed, lane, where, column):
    return jnp.where(lane == where, column, packed)


def expand_kernel(total_ref, basis_ref, local_ref, inverse_ref, source_ref, field_ref, low_ref, high_ref):
    x = pl.program_id(0)
    _, rows, cells, rank = basis_ref.shape
    chains = total_ref.shape[0]
    coef = total_ref[...].astype(jnp.bfloat16)
    basis = basis_ref[...].reshape(rows * cells, rank)
    corr = lax.dot_general(coef, basis, (((1,), (1,)), ((), ())), preferred_element_type=jnp.float32)
    lane = lax.broadcasted_iota(jnp.int32, low_ref.shape, 1)
    low, high = low_ref[...], high_ref[...]
    for y in range(rows):
        source = local_ref[0, y] + corr[:, y * cells:(y + 1) * cells]
        field = source * inverse_ref[0, y:y + 1, :]
        source_ref[0, y] = source
        field_ref[0, y] = field
        low = put_column(low, lane, x * rows + y, field[:, :1])
        high = put_column(high, lane, x * rows + y, field[:, cells - 1:])
    low_ref[...] = low
    high_ref[...] = high


def expand(total, basis, local, inverse):
    planes, rows, cells, rank = basis.shape
    chains = total.shape[0]
    whole = jax.ShapeDtypeStruct((planes, rows, chains, cells), jnp.float32)
    face = jax.ShapeDtypeStruct((chains, planes * rows), jnp.float32)
    return pl.pallas_call(
        expand_kernel,
        grid=(planes,),
        in_specs=[
            pl.BlockSpec((chains, rank), lambda x: (0, 0)),
            pl.BlockSpec((1, rows, cells, rank), lambda x: (x, 0, 0, 0)),
            pl.BlockSpec((1, rows, chains, cells), lambda x: (x, 0, 0, 0)),
            pl.BlockSpec((1, rows, cells), lambda x: (x, 0, 0)),
        ],
        out_specs=[
            pl.BlockSpec((1, rows, chains, cells), lambda x: (x, 0, 0, 0)),
            pl.BlockSpec((1, rows, chains, cells), lambda x: (x, 0, 0, 0)),
            pl.BlockSpec((chains, planes * rows), lambda x: (0, 0)),
            pl.BlockSpec((chains, planes * rows), lambda x: (0, 0)),
        ],
        out_shape=[whole, whole, face, face],
        name="expand",
        compiler_params=pltpu.CompilerParams(vmem_limit_bytes=24 * 2**20),
    )(total, basis, local, inverse)


def new_field(refs, x, y, lane):
    mask_ref, field_ref, source_ref, inverse_ref, xlow_ref, xhigh_ref, ylow_ref, yhigh_ref, zlow_ref, zhigh_ref = refs
    planes, rows, chains, cells = field_ref.shape
    here = field_ref[x, y]
    place = x * rows + y
    value = source_ref[x, y]
    value = value + (field_ref[x + 1, y] if x + 1 < planes else xhigh_ref[0, y])
    value = value + (field_ref[x - 1, y] if x > 0 else xlow_ref[0, y])
    value = value + (field_ref[x, y + 1] if y + 1 < rows else yhigh_ref[x, 0] * mask_ref[1])
    value = value + (field_ref[x, y - 1] if y > 0 else ylow_ref[x, 0] * mask_ref[0])
    value = value + jnp.where(lane == 0, zlow_ref[:, place:place + 1], pltpu.roll(here, 1, 1))
    value = value + jnp.where(lane == cells - 1, zhigh_ref[:, place:place + 1], pltpu.roll(here, cells - 1, 1))
    return value * inverse_ref[x, y:y + 1, :]


def sweep_kernel(*refs):
    *inputs, out_ref, low_ref, high_ref = refs
    planes, rows, chains, cells = out_ref.shape
    lane = lax.broadcasted_iota(jnp.int32, (chains, cells), 1)
    face_lane = lax.broadcasted_iota(jnp.int32, low_ref.shape, 1)
    low = jnp.zeros(low_ref.shape, jnp.float32)
    high = jnp.zeros(high_ref.shape, jnp.float32)
    for x in range(planes):
        for y in range(rows):
            value = new_field(inputs, x, y, lane)
            out_ref[x, y] = value
            low = put_column(low, face_lane, x * rows + y, value[:, :1])
            high = put_column(high, face_lane, x * rows + y, value[:, cells - 1:])
    low_ref[...] = low
    high_ref[...] = high


def last_kernel(*refs):
    *inputs, current_ref, out_ref = refs
    chains, planes, rows, cells = out_ref.shape
    lane = lax.broadcasted_iota(jnp.int32, (chains, cells), 1)
    for x in range(planes):
        plane = jnp.stack([new_field(inputs, x, y, lane) for y in range(rows)])
        out_ref[:, x] = current_ref[:, x] + jnp.swapaxes(plane, 0, 1)


def specs(count):
    return [pl.BlockSpec(memory_space=pltpu.SMEM)] + [pl.BlockSpec(memory_space=pltpu.VMEM)] * count


def near(*arrays):
    return [pltpu.with_memory_space_constraint(a, pltpu.VMEM) for a in arrays]


def halo(field, low, high):
    forward, backward = lines("gx")
    xlow = lax.ppermute(field[-1:], "gx", forward)
    xhigh = lax.ppermute(field[:1], "gx", backward)
    forward, backward = lines("gz")
    zlow = lax.ppermute(high, "gz", forward)
    zhigh = lax.ppermute(low, "gz", backward)
    if lax.axis_size("gy") == 2:
        send = jnp.where(lax.axis_index("gy") == 0, field[:, -1:], field[:, :1])
        ylow = yhigh = lax.ppermute(send, "gy", [(0, 1), (1, 0)])
    else:
        forward, backward = lines("gy")
        ylow = lax.ppermute(field[:, -1:], "gy", forward)
        yhigh = lax.ppermute(field[:, :1], "gy", backward)
    return xlow, xhigh, ylow, yhigh, zlow, zhigh


def body(gradient, noise_draw, current, eigvectors, eigvalues, reaction):
    chains = gradient.shape[0]
    rank = eigvectors.shape[3]
    cells = reaction.size
    basis = eigvectors.reshape(cells, rank)
    stacked = jnp.concatenate(
        [gradient.reshape(chains, cells), noise_draw.reshape(chains, cells)], 0
    )
    partial_sums = jnp.dot(stacked, basis, preferred_element_type=jnp.float32)
    damp = eigvalues / (eigvalues + 1.0)
    root_damp = 1.0 - 1.0 / jnp.sqrt(1.0 + eigvalues)
    total = 0.5 * damp * partial_sums[:chains] - 1.0 * root_damp * partial_sums[chains:]
    for axis in ("gy", "gz", "gx"):
        total = reduce_over(total, axis)
    local = -0.5 * gradient.astype(jnp.float32) + 1.0 * noise_draw.astype(jnp.float32)
    local = jnp.transpose(local, (1, 2, 0, 3))
    inverse = 1.0 / (reaction + 6.0)
    last = lax.axis_size("gy") - 1
    place = lax.axis_index("gy")
    mask = jnp.where(jnp.arange(2) == 0, place > 0, place < last).astype(jnp.float32)

    source, field, low, high = expand(total, eigvectors, local, inverse)
    for _ in range(SWEEPS - 2):
        field, low, high = pl.pallas_call(
            sweep_kernel,
            in_specs=specs(9),
            out_specs=[pl.BlockSpec(memory_space=pltpu.VMEM)] * 3,
            out_shape=[pltpu.VMEM(a.shape, jnp.float32) for a in (field, low, high)],
            name="sweep",
            compiler_params=pltpu.CompilerParams(vmem_limit_bytes=16 * 2**20),
        )(mask, *near(field, source, inverse, *halo(field, low, high)))
    return pl.pallas_call(
        last_kernel,
        in_specs=specs(10),
        out_specs=pl.BlockSpec(memory_space=pltpu.VMEM),
        out_shape=jax.ShapeDtypeStruct(current.shape, jnp.float32),
        name="last_sweep",
        compiler_params=pltpu.CompilerParams(vmem_limit_bytes=16 * 2**20),
    )(mask, *near(field, source, inverse, *halo(field, low, high), current))


def solution(mesh):
    return jax.shard_map(
        body,
        mesh=mesh,
        in_specs=(
            P(None, "gx", "gy", "gz"),
            P(None, "gx", "gy", "gz"),
            P(None, "gx", "gy", "gz"),
            P("gx", "gy", "gz", None),
            P(),
            P("gx", "gy", "gz"),
        ),
        out_specs=P(None, "gx", "gy", "gz"),
        check_vma=False,
    )
```

```python
import jax
import jax.numpy as jnp
from jax import lax
from jax.experimental import pallas as pl
from jax.experimental.pallas import tpu as pltpu
from jax.sharding import PartitionSpec as P

SWEEPS = 4


def reduce_over(value, axis):
    count = lax.axis_size(axis)
    if count & (count - 1):
        return lax.psum(value, axis)
    step = 1
    while step < count:
        value = value + lax.ppermute(value, axis, [(i, i ^ step) for i in range(count)])
        step *= 2
    return value


def lines(axis):
    count = lax.axis_size(axis)
    forward = [(i, i + 1) for i in range(count - 1)]
    return forward, [(target, source) for source, target in forward]


def put_faces(packed, field, plane):
    rows, chains, cells = field.shape
    slots = cells // 2
    pair = lax.broadcasted_iota(jnp.int32, (chains, cells), 1) // 2
    for y in range(rows):
        group, slot = divmod(plane * rows + y, slots)
        turned = pltpu.roll(field[y], (2 * slot + 1) % cells, 1)
        packed[group] = jnp.where(pair == slot, turned, packed[group])


def blank_faces(faces_ref):
    return [jnp.zeros(faces_ref.shape[1:], jnp.float32) for _ in range(faces_ref.shape[0])]


def slab_copies(basis_hbm, basis_ref, sems):
    return [
        pltpu.make_async_copy(basis_hbm.at[x], basis_ref.at[x], sems.at[x])
        for x in range(basis_ref.shape[0])
    ]


def project_kernel(
    gradient_hbm, noise_hbm, basis_hbm, eigvalues_ref, mixed_ref,
    gradient_ref, noise_ref, basis_ref, data_sems, basis_sems,
):
    planes, rows, cells, rank = basis_ref.shape
    chains = mixed_ref.shape[0]
    data = [
        pltpu.make_async_copy(gradient_hbm, gradient_ref, data_sems.at[0]),
        pltpu.make_async_copy(noise_hbm, noise_ref, data_sems.at[1]),
    ]
    slabs = slab_copies(basis_hbm, basis_ref, basis_sems)
    for copy in data + slabs:
        copy.start()
    for copy in data:
        copy.wait()
    sums = jnp.zeros((2 * chains, rank), jnp.float32)
    for x in range(planes):
        gradient = jnp.swapaxes(gradient_ref[:, x].astype(jnp.float32), 0, 1)
        noise = jnp.swapaxes(noise_ref[:, x].astype(jnp.float32), 0, 1)
        stacked = jnp.concatenate([gradient, noise], 1).astype(jnp.bfloat16)
        stacked = jnp.concatenate([stacked[y] for y in range(rows)], 1)
        slabs[x].wait()
        slab = basis_ref[x].reshape(rows * cells, rank)
        sums = sums + jnp.dot(stacked, slab, preferred_element_type=jnp.float32)
    values = eigvalues_ref[...]
    damp = values / (values + 1.0)
    root_damp = 1.0 - 1.0 / jnp.sqrt(1.0 + values)
    mixed_ref[...] = 0.5 * damp * sums[:chains] - 1.0 * root_damp * sums[chains:]


def project(gradient, noise_draw, eigvectors, eigvalues):
    planes, rows, cells, rank = eigvectors.shape
    chains = gradient.shape[0]
    outside = pl.BlockSpec(memory_space=pltpu.HBM)
    inside = pl.BlockSpec(memory_space=pltpu.VMEM)
    return pl.pallas_call(
        project_kernel,
        in_specs=[outside, outside, outside, inside],
        out_specs=inside,
        out_shape=pltpu.VMEM((chains, rank), jnp.float32),
        scratch_shapes=[
            pltpu.VMEM(gradient.shape, gradient.dtype),
            pltpu.VMEM(noise_draw.shape, noise_draw.dtype),
            pltpu.VMEM(eigvectors.shape, eigvectors.dtype),
            pltpu.SemaphoreType.DMA((2,)),
            pltpu.SemaphoreType.DMA((planes,)),
        ],
        compiler_params=pltpu.CompilerParams(vmem_limit_bytes=60 * 2**20),
        name="project",
    )(gradient, noise_draw, eigvectors, eigvalues.reshape(1, rank))


def expand_kernel(
    total_ref, basis_hbm, local_ref, inverse_ref, source_ref, field_ref, faces_ref, basis_ref, sems
):
    planes, rows, cells, rank = basis_ref.shape
    slabs = slab_copies(basis_hbm, basis_ref, sems)
    for copy in slabs:
        copy.start()
    coef = total_ref[...].astype(jnp.bfloat16)
    faces = blank_faces(faces_ref)
    for x in range(planes):
        slabs[x].wait()
        slab = basis_ref[x].reshape(rows * cells, rank)
        corr = lax.dot_general(coef, slab, (((1,), (1,)), ((), ())), preferred_element_type=jnp.float32)
        corr = jnp.stack([corr[:, y * cells:(y + 1) * cells] for y in range(rows)])
        source = local_ref[x] + corr
        field = source * inverse_ref[x][:, None, :]
        put_faces(faces, field, x)
        source_ref[x] = source
        field_ref[x] = field
    for group, face in enumerate(faces):
        faces_ref[group] = face


def new_plane(refs, x, edges):
    mask_ref, field_ref, source_ref, inverse_ref, xlow_ref, xhigh_ref, ylow_ref, yhigh_ref, zlow_ref, zhigh_ref = refs
    planes, rows, chains, cells = field_ref.shape
    here = field_ref[x]
    value = source_ref[x]
    value = value + (field_ref[x + 1] if x + 1 < planes else xhigh_ref[0])
    value = value + (field_ref[x - 1] if x > 0 else xlow_ref[0])
    value = value + jnp.concatenate([here[1:], yhigh_ref[x] * mask_ref[1]], 0)
    value = value + jnp.concatenate([ylow_ref[x] * mask_ref[0], here[:-1]], 0)
    slots = cells // 2
    outer = []
    for y in range(rows):
        group, slot = divmod(x * rows + y, slots)
        outer.append(pltpu.roll(edges[group], (-2 * slot - 1) % cells, 1))
    outer = jnp.concatenate(outer, 0)
    flat = here.reshape(rows * chains, cells)
    lane = lax.broadcasted_iota(jnp.int32, flat.shape, 1)
    total = jnp.where(lane == 0, outer, pltpu.roll(flat, 1, 1))
    total = total + jnp.where(lane == cells - 1, outer, pltpu.roll(flat, cells - 1, 1))
    return (value + total.reshape(rows, chains, cells)) * inverse_ref[x][:, None, :]


def both_edges(zlow_ref, zhigh_ref):
    groups, chains, cells = zlow_ref.shape
    even = lax.broadcasted_iota(jnp.int32, (chains, cells), 1) % 2 == 0
    return [
        jnp.where(even, pltpu.roll(zhigh_ref[g], cells - 1, 1), pltpu.roll(zlow_ref[g], 1, 1))
        for g in range(groups)
    ]


def sweep_kernel(*refs):
    *inputs, out_ref, faces_ref = refs
    edges = both_edges(*inputs[-2:])
    faces = blank_faces(faces_ref)
    for x in range(out_ref.shape[0]):
        plane = new_plane(inputs, x, edges)
        out_ref[x] = plane
        put_faces(faces, plane, x)
    for group, face in enumerate(faces):
        faces_ref[group] = face


def last_kernel(*refs):
    *inputs, current_ref, out_ref = refs
    edges = both_edges(*inputs[-2:])
    for x in range(out_ref.shape[1]):
        out_ref[:, x] = current_ref[:, x] + jnp.swapaxes(new_plane(inputs, x, edges), 0, 1)


def specs(count):
    return [pl.BlockSpec(memory_space=pltpu.SMEM)] + [pl.BlockSpec(memory_space=pltpu.VMEM)] * count


def near(*arrays):
    return [pltpu.with_memory_space_constraint(a, pltpu.VMEM) for a in arrays]


def halo(field, faces):
    forward, backward = lines("gz")
    zlow = lax.ppermute(faces, "gz", forward)
    zhigh = lax.ppermute(faces, "gz", backward)
    forward, backward = lines("gx")
    xlow = lax.ppermute(field[-1:], "gx", forward)
    xhigh = lax.ppermute(field[:1], "gx", backward)
    if lax.axis_size("gy") == 2:
        send = jnp.where(lax.axis_index("gy") == 0, field[:, -1:], field[:, :1])
        ylow = yhigh = lax.ppermute(send, "gy", [(0, 1), (1, 0)])
    else:
        forward, backward = lines("gy")
        ylow = lax.ppermute(field[:, -1:], "gy", forward)
        yhigh = lax.ppermute(field[:, :1], "gy", backward)
    return xlow, xhigh, ylow, yhigh, zlow, zhigh


def body(gradient, noise_draw, current, eigvectors, eigvalues, reaction):
    chains = gradient.shape[0]
    planes, rows, cells, rank = eigvectors.shape
    last = lax.axis_size("gy") - 1
    place = lax.axis_index("gy")
    mask = jnp.where(jnp.arange(2) == 0, place > 0, place < last).astype(jnp.float32)
    total = project(gradient, noise_draw, eigvectors, eigvalues)
    for axis in ("gy", "gz", "gx"):
        total = reduce_over(total, axis)
    local = -0.5 * gradient.astype(jnp.float32) + 1.0 * noise_draw.astype(jnp.float32)
    local = jnp.transpose(local, (1, 2, 0, 3))
    inverse = 1.0 / (reaction + 6.0)
    total, local, inverse = near(total, local, inverse)

    inside = pl.BlockSpec(memory_space=pltpu.VMEM)
    limit = pltpu.CompilerParams(vmem_limit_bytes=16 * 2**20)
    whole = pltpu.VMEM((planes, rows, chains, cells), jnp.float32)
    packed = pltpu.VMEM((-(-2 * planes * rows // cells), chains, cells), jnp.float32)
    source, field, faces = pl.pallas_call(
        expand_kernel,
        in_specs=[inside, pl.BlockSpec(memory_space=pltpu.HBM), inside, inside],
        out_specs=[inside] * 3,
        out_shape=[whole, whole, packed],
        scratch_shapes=[
            pltpu.VMEM(eigvectors.shape, eigvectors.dtype),
            pltpu.SemaphoreType.DMA((planes,)),
        ],
        compiler_params=pltpu.CompilerParams(vmem_limit_bytes=56 * 2**20),
        name="expand",
    )(total, eigvectors, local, inverse)
    for _ in range(SWEEPS - 2):
        field, faces = pl.pallas_call(
            sweep_kernel,
            in_specs=specs(9),
            out_specs=[inside] * 2,
            out_shape=[whole, packed],
            compiler_params=limit,
            name="sweep",
        )(mask, *near(field, source, inverse, *halo(field, faces)))
    return pl.pallas_call(
        last_kernel,
        in_specs=specs(10),
        out_specs=inside,
        out_shape=jax.ShapeDtypeStruct(current.shape, jnp.float32),
        compiler_params=limit,
        name="last_sweep",
    )(mask, *near(field, source, inverse, *halo(field, faces), current))


def solution(mesh):
    return jax.shard_map(
        body,
        mesh=mesh,
        in_specs=(
            P(None, "gx", "gy", "gz"),
            P(None, "gx", "gy", "gz"),
            P(None, "gx", "gy", "gz"),
            P("gx", "gy", "gz", None),
            P(),
            P("gx", "gy", "gz"),
        ),
        out_specs=P(None, "gx", "gy", "gz"),
        check_vma=False,
    )
```
